32 devices in a mesh: wide: 8 (over z, y), narrow: 2 (over x), grp: 2 (over core).
Axes of the slice: x: 2, y: 2, z: 4, core: 2. Of those that a mesh axis runs over, the one named last changes fastest.
Arguments:
- boundary_block: float32 [8, 2048, 16384], P(None, ('narrow', 'grp'), 'wide'), may hold values from -4 to 4
- schur_blocks: float32 [2, 1536, 1536], P('narrow', ('wide', 'grp')), may hold values from -2 to 2
- interface_rows: int32 [2, 1536], P('narrow'), may hold values from 0 to 8191, as said below
- live_rows: int32 [2], P('narrow'), may hold values from 1 to 1536, 2304 in all
- row_scale: float32 [8, 2048], P('wide', ('narrow', 'grp')), may hold values from 0.4 to 1.2
- excitation: float32 [8, 2048, 128], P('wide', ('narrow', 'grp')), may hold values from -6 to 6
Outputs:
- traces: float32 [8, 2048, 128], P('wide', ('narrow', 'grp'))
- residual: float32 [8, 2048, 128], P('wide', ('narrow', 'grp'))
The draws below stay inside these ranges and needn't reach their ends.
Inputs may be any that keep to these rules, and one draw needn't show every extreme that they name: `interface_rows`: each substructure's row holds 1536 different positions, 0 to 8191; within each aligned block of 96 slots, at most 32 positions lie in one aligned range of 512 positions, and every substructure reaches 32 in some block.
All inputs are finite; a program needn't handle non-finite values. No bound on the sum of `live_rows` on one device may be relied on, other than what follows from the above.
Results may differ from the reference program's by a relative error of at most 0.00016.
Values sent between devices are 32-bit elements; how exact they have to be, the bound alone decides.
No kernel may reach another device: no remote copies, remote signals or barrier semaphores. Data moves between devices by JAX's collectives and lax.ppermute only.
A program may use at most 128 MiB of HBM per device.

```python
import math
import jax
import jax.numpy as jnp
import numpy as np
from jax import lax

NB = 16384
M = 1536
SUB_PAN = 1
R = 128
ITERS = 3
NSUB = 2
PANEL = 8192
N_WIDE = 8
N_NARROW = 2
N_GRP = 2


def draw_boundary_block(key, part):
    spread = jax.random.normal(key, (NB, NB), jnp.float32)
    matrix = jnp.eye(NB, dtype=jnp.float32) + spread * (0.5 / NB ** 0.5)
    return matrix.T.reshape(N_WIDE, NB // N_WIDE, NB)


def draw_schur_blocks(key, part):
    spread = jax.random.normal(key, (NSUB, M, M), jnp.float32)
    return 0.25 * jnp.eye(M, dtype=jnp.float32)[None] + spread * (0.12 / M ** 0.5)


def draw_interface_rows(key, part):
    blocks = N_WIDE * N_GRP
    piece = PANEL // blocks
    keys = jax.random.split(jax.random.fold_in(key, 7), NSUB)
    places = jnp.arange(PANEL, dtype=jnp.int32)
    counter = jnp.arange(M, dtype=jnp.int32)
    slot_of = counter % blocks * (M // blocks) + counter // blocks

    def one(single):
        first, second = jax.random.split(single)
        ranks = jax.random.permutation(first, PANEL).astype(jnp.int32)
        whole_owner = jax.random.randint(second, (), 0, blocks, dtype=jnp.int32)
        scores = ranks - jnp.where(places // piece == whole_owner, PANEL, 0).astype(jnp.int32)
        chosen = jnp.argsort(scores, stable=True)[:M].astype(jnp.int32)
        by_owner = chosen[jnp.argsort(chosen // piece, stable=True)]
        return jnp.zeros((M,), jnp.int32).at[slot_of].set(by_owner)
    return jax.vmap(one)(keys).astype(jnp.int32)


def block_levels(own_key, extent, pieces, least, high):
    level, own = 1.0, jax.random.fold_in(own_key, 6)
    for axis_at, parts in pieces:
        steps = jnp.exp(jax.random.uniform(jax.random.fold_in(own, axis_at), (parts,), jnp.float32, least / len(pieces), high / len(pieces)))
        level = level * jnp.repeat(steps, extent[axis_at] // parts).reshape([-1 if axis == axis_at else 1 for axis in range(len(extent))])
    return level


def profile(number_of, total, limit, skew):
    portions = [(1 << 20) // math.isqrt(standing ** skew) + 1 for standing in range(2, number_of + 1)]
    spare, given = total - limit - (number_of - 1), [1] * (number_of - 1)
    while spare > 0:
        candidates = [i for i in range(number_of - 1) if given[i] < limit]
        pool, left = sum([portions[i] for i in candidates]), spare
        for i in candidates:
            more = min(limit - given[i], max(1, left * portions[i] // pool), spare)
            given[i] = given[i] + more
            spare = spare - more
    return np.array([limit] + given)


def ragged_sizes(own_key, count, total, bound, lean):
    if count == 2:
        one = jax.random.randint(own_key, (), max(1, total - bound), min(bound, total - 1) + 1)
        return jnp.stack([one, total - one])
    tallies = jnp.asarray(profile(count, total, bound, lean), jnp.int32)
    twos = (count - 1) // 2
    source_of, sink = tallies[1:1 + 2 * twos:2], tallies[2:2 + 2 * twos:2]
    room = jnp.minimum(source_of - 1, bound - sink)
    shifted = jax.random.randint(jax.random.fold_in(own_key, 1), (twos,), 0, 1 << 20) % (room + 1)
    tallies = tallies.at[1:1 + 2 * twos:2].set(source_of - shifted).at[2:2 + 2 * twos:2].set(sink + shifted)
    return tallies[jax.random.permutation(jax.random.fold_in(own_key, 2), count)]


def normal_values(key, shape, deviation, most, shards=(), kind=jnp.bfloat16):
    entries = jax.random.normal(key, shape, jnp.float32) * deviation
    if len(shards) > 0:
        entries = block_levels(key, shape, shards, -0.22, 0.18) * entries
    return jnp.clip(entries, min=-most, max=most).astype(kind)


def setup_inputs(seed: int = 0) -> dict:
    key_list = jax.random.split(jax.random.key(seed), 7)
    return {
        "boundary_block": draw_boundary_block(jax.random.fold_in(key_list[6], 71), 0),
        "schur_blocks": draw_schur_blocks(jax.random.fold_in(key_list[6], 71), 0),
        "interface_rows": draw_interface_rows(jax.random.fold_in(key_list[6], 71), 0),
        "live_rows": ragged_sizes(key_list[3], NSUB, NSUB * M * 3 // 4, M, 2).astype(jnp.int32),
        "row_scale": jnp.clip(jnp.exp(math.log(1.2) - 1.0986123 * jax.random.uniform(key_list[4], (N_WIDE, NB // N_WIDE), jnp.float32) ** block_levels(key_list[4], (N_WIDE, NB // N_WIDE), ((0, 8), (1, 4)), -0.2, 0.2)), 0.4, 1.2),
        "excitation": normal_values(key_list[5], (N_WIDE, NB // N_WIDE, R), 1.0, 6.0, ((0, 8), (1, 4)), jnp.float32),
    }


RELAX = 0.35


def reference(boundary_block, schur_blocks, interface_rows, live_rows, row_scale, excitation):
    column_major = boundary_block.reshape(NB, NB)
    row_weight = row_scale.reshape(NB, 1)
    forcing = excitation.reshape(NB, R)
    strip_width = NB // (N_WIDE * N_NARROW)
    panel_index = jnp.arange(NSUB, dtype=jnp.int32) // SUB_PAN
    global_rows = ((interface_rows // strip_width) * (NB // N_WIDE) + panel_index[:, None] * strip_width + interface_rows % strip_width).astype(jnp.int32)
    positions = jnp.arange(M, dtype=jnp.int32)
    live_mask = (positions[None, :] < live_rows[:, None]).astype(jnp.float32)

    def operate(current):
        boundary = lax.dot_general(column_major, current, (((0,), (0,)), ((), ())), precision=lax.Precision.HIGHEST, preferred_element_type=jnp.float32)

        def add_one(totals, inputs):
            schur, targets, weights = inputs
            local = current[targets] * weights[:, None]
            result = jnp.dot(schur, local, precision=lax.Precision.HIGHEST, preferred_element_type=jnp.float32) * weights[:, None]
            return totals.at[targets].add(result), None

        interface, unused = lax.scan(add_one, jnp.zeros((NB, R), jnp.float32), (schur_blocks, global_rows, live_mask))
        return boundary + interface

    traces = RELAX * row_weight * forcing
    residual = forcing
    for sweep in range(ITERS):
        residual = forcing - operate(traces)
        traces = traces + RELAX * row_weight * residual
    return traces.reshape(N_WIDE, NB // N_WIDE, R), residual.reshape(N_WIDE, NB // N_WIDE, R)
```

```python
import jax
import jax.numpy as jnp
from jax import lax
from jax.experimental import pallas as pl
from jax.experimental.pallas import tpu as pltpu
from jax.sharding import PartitionSpec as P

ITERS = 3


RELAX = 0.35

CHUNK = 256
F32 = jnp.float32
BF16 = jnp.bfloat16


def split(value):
    high = value.astype(BF16)
    return high, (value - high.astype(F32)).astype(BF16)


def slot_ranks(owners):
    count = owners.shape[-1]
    same = owners[..., :, None] == owners[..., None, :]
    earlier = jnp.arange(count)[None, :] < jnp.arange(count)[:, None]
    return jnp.sum((same & earlier).astype(jnp.int32), axis=-1)


def vmem():
    return pl.BlockSpec(memory_space=pltpu.VMEM)


def smem():
    return pl.BlockSpec(memory_space=pltpu.SMEM)


def begin(row_scale, excitation):
    piece, batch = excitation.shape

    def body(scale_ref, excitation_ref, forcing_ref, weight_ref, traces_ref):
        weight_ref[...] = RELAX * scale_ref[...]
        forcing_ref[...] = excitation_ref[...].T
        traces_ref[...] = RELAX * scale_ref[...] * forcing_ref[...]

    wide = jax.ShapeDtypeStruct((batch, piece), F32)
    return pl.pallas_call(
        body,
        out_shape=(wide, jax.ShapeDtypeStruct((1, piece), F32), wide),
        in_specs=[vmem()] * 2,
        out_specs=(vmem(),) * 3,
        compiler_params=pltpu.CompilerParams(vmem_limit_bytes=4 << 20),
        name="begin",
    )(row_scale, excitation)


def tile_terms(boundary_block, first_chunk, many):
    strips, piece, rows = boundary_block.shape
    width = many * CHUNK
    depth = 4

    def body(b_ref, *refs):
        high_refs, low_refs = refs[:many], refs[many : 2 * many]
        buf, sems = refs[2 * many :]

        def copy(step):
            return pltpu.make_async_copy(
                b_ref.at[step, :, pl.ds(first_chunk * CHUNK, width)], buf.at[step % depth], sems.at[step % depth]
            )

        for step in range(depth):
            copy(step).start()
        for step in range(strips):
            copy(step).wait()
            inner = pl.ds((step % 2) * piece, piece)
            for n in range(many):
                high, low = split(buf[step % depth, :, n * CHUNK : (n + 1) * CHUNK])
                high_refs[n][step // 2, inner] = high
                low_refs[n][step // 2, inner] = low
            if step + depth < strips:
                copy(step + depth).start()

    out = jax.ShapeDtypeStruct((strips // 2, 2 * piece, CHUNK), BF16)
    terms = pl.pallas_call(
        body,
        out_shape=(out,) * (2 * many),
        in_specs=[pl.BlockSpec(memory_space=pltpu.HBM)],
        out_specs=(vmem(),) * (2 * many),
        scratch_shapes=[pltpu.VMEM((depth, piece, width), F32), pltpu.SemaphoreType.DMA((depth,))],
        compiler_params=pltpu.CompilerParams(vmem_limit_bytes=10 << 20),
        cost_estimate=pl.CostEstimate(flops=10**9, bytes_accessed=0, transcendentals=0),
        name="tile_terms",
    )(boundary_block)
    return terms[:many], terms[many:]


def schur_terms(schur_own, schur_other, column_of, grp_index, strips, piece):
    share, slots = schur_own.shape
    half = CHUNK // 2

    def body(grp_ref, col_ref, own_ref, other_ref, high_ref, low_ref, s_high, s_low):
        s_high[...] = jnp.zeros(s_high.shape, BF16)
        s_low[...] = jnp.zeros(s_low.shape, BF16)
        group = grp_ref[0]
        for ref, at in ((own_ref, group), (other_ref, 1 - group)):
            high, low = split(ref[...])
            where = pl.ds(pl.multiple_of(at * half, half), share)
            s_high[where, :] = high
            s_low[where, :] = low

        def one(strip, carry):
            place = lax.broadcasted_iota(jnp.int32, (piece, slots), 0) + strip * piece
            hot = (place == col_ref[...]).astype(F32).astype(BF16)
            inner = pl.ds(pl.multiple_of(lax.rem(strip, 2) * piece, piece), piece)
            for term, out in ((s_high, high_ref), (s_low, low_ref)):
                value = lax.dot_general(hot, term[...], (((1,), (1,)), ((), ())), preferred_element_type=F32)
                out[strip // 2, inner] = value.astype(BF16)
            return carry

        lax.fori_loop(0, strips, one, 0)

    out = jax.ShapeDtypeStruct((strips // 2, 2 * piece, CHUNK), BF16)
    return pl.pallas_call(
        body,
        out_shape=(out, out),
        in_specs=[smem()] + [vmem()] * 3,
        out_specs=(vmem(),) * 2,
        scratch_shapes=[pltpu.VMEM((CHUNK, slots), BF16)] * 2,
        compiler_params=pltpu.CompilerParams(vmem_limit_bytes=10 << 20),
        cost_estimate=pl.CostEstimate(flops=2 * 10**9, bytes_accessed=0, transcendentals=0),
        name="schur_terms",
    )(grp_index, column_of, schur_own, schur_other)


def multiply(blocks, outer_of, place_of, grp_index, high, low, before, main_rows=True, side_rows=True):
    chunks = len(high) - 1
    pairs = len(blocks) // 2
    batch, piece = blocks[0].shape
    per_piece = piece // CHUNK
    kept = chunks // 2
    wanted = (list(range(chunks)) if main_rows else []) + ([chunks] if side_rows else [])

    def body(outer_ref, place_ref, grp_ref, *refs):
        take = iter(refs)
        block_refs = [next(take) for _ in range(2 * pairs)]
        high_refs = {n: next(take) for n in wanted}
        low_refs = {n: next(take) for n in wanted}
        old = [next(take) for _ in before]
        if main_rows:
            keep_ref, send_ref = next(take), next(take)
        if side_rows:
            side_ref = next(take)
        both, full = take
        group = grp_ref[0]
        swapped = place_ref[0]
        for j in range(2 * pairs):
            first, second = split(block_refs[j][...])
            at = pl.ds(pl.multiple_of(lax.rem(j + swapped, 2) * piece, piece), piece)
            both[j // 2, 0:batch, at] = first
            both[j // 2, batch : 2 * batch, at] = second

        def product(n):
            total = None
            for j in range(pairs):
                outer = outer_ref[j]
                top = jnp.dot(both[j], high_refs[n][outer], preferred_element_type=F32)
                bottom = jnp.dot(both[j, 0:batch, :], low_refs[n][outer], preferred_element_type=F32)
                value = top[:batch] + (top[batch:] + bottom)
                total = value if total is None else total + value
            return total

        if side_rows:
            value = product(chunks)
            side_ref[...] = old[-1][...] + value if before else value
        if main_rows:
            for n in range(chunks):
                full[n] = product(n)
            for m in range(kept):
                base = (m // per_piece) * 2 * per_piece + m % per_piece
                stays, goes = full[base + group * per_piece], full[base + (1 - group) * per_piece]
                keep_ref[m] = old[0][m] + stays if before else stays
                send_ref[m] = old[1][m] + goes if before else goes

    main = jax.ShapeDtypeStruct((kept, batch, CHUNK), F32)
    side = jax.ShapeDtypeStruct((batch, CHUNK), F32)
    flops = 6 * pairs * 2 * piece * batch * CHUNK * len(wanted)
    outs = ((main, main) if main_rows else ()) + ((side,) if side_rows else ())
    return pl.pallas_call(
        body,
        out_shape=outs,
        in_specs=[smem()] * 3 + [vmem()] * (2 * pairs + 2 * len(wanted) + len(before)),
        out_specs=(vmem(),) * len(outs),
        scratch_shapes=[
            pltpu.VMEM((pairs, 2 * batch, 2 * piece), BF16),
            pltpu.VMEM((chunks, batch, CHUNK), F32),
        ],
        compiler_params=pltpu.CompilerParams(vmem_limit_bytes=6 << 20),
        cost_estimate=pl.CostEstimate(flops=flops, bytes_accessed=0, transcendentals=0),
        name="multiply",
    )(outer_of, place_of, grp_index, *blocks, *(high[n] for n in wanted), *(low[n] for n in wanted), *before)


def gather_half(keep, got, narrow_index):
    kept, batch, _ = keep.shape
    mine = kept // 2

    def body(narrow_ref, keep_ref, got_ref, send_ref, stay_ref):
        panel = narrow_ref[0]
        for m in range(mine):
            send_ref[m] = keep_ref[(1 - panel) * mine + m] + got_ref[(1 - panel) * mine + m]
            stay_ref[m] = keep_ref[panel * mine + m] + got_ref[panel * mine + m]

    part = jax.ShapeDtypeStruct((mine, batch, CHUNK), F32)
    return pl.pallas_call(
        body,
        out_shape=(part, part),
        in_specs=[smem()] + [vmem()] * 2,
        out_specs=(vmem(),) * 2,
        compiler_params=pltpu.CompilerParams(vmem_limit_bytes=4 << 20),
        cost_estimate=pl.CostEstimate(flops=2 * 10**8, bytes_accessed=0, transcendentals=0),
        name="gather_half",
    )(narrow_index, keep, got)


def pick_rows(side, got_side, pick, target_of):
    outer, twice, _ = pick.shape
    cap = twice // 2
    batch = side.shape[0]

    def body(target_ref, side_ref, got_ref, pick_ref, own_ref, other_ref):
        first, second = split(side_ref[...] + got_ref[...])
        dims = (((1,), (1,)), ((), ()))
        for by in range(outer):
            chosen = pick_ref[target_ref[by]]
            rows = lax.dot_general(chosen, first, dims, preferred_element_type=F32)
            rows += lax.dot_general(chosen, second, dims, preferred_element_type=F32)
            own_ref[by] = rows[:cap]
            other_ref[by] = rows[cap:]

    rows = jax.ShapeDtypeStruct((outer, cap, batch), F32)
    return pl.pallas_call(
        body,
        out_shape=(rows, rows),
        in_specs=[smem()] + [vmem()] * 3,
        out_specs=(vmem(),) * 2,
        compiler_params=pltpu.CompilerParams(vmem_limit_bytes=4 << 20),
        cost_estimate=pl.CostEstimate(flops=2 * 10**8, bytes_accessed=0, transcendentals=0),
        name="pick_rows",
    )(target_of, side, got_side, pick)


def join_rows(own, got):
    outer, cap, batch = own.shape

    def body(own_ref, got_ref, *outs):
        for by in range(outer):
            outs[by][0:cap, :] = own_ref[by]
            outs[by][cap : 2 * cap, :] = got_ref[by]

    return pl.pallas_call(
        body,
        out_shape=(jax.ShapeDtypeStruct((2 * cap, batch), F32),) * outer,
        in_specs=[vmem()] * 2,
        out_specs=(vmem(),) * outer,
        compiler_params=pltpu.CompilerParams(vmem_limit_bytes=4 << 20),
        cost_estimate=pl.CostEstimate(flops=10**8, bytes_accessed=0, transcendentals=0),
        name="join_rows",
    )(own, got)


def update(stay, got, rows, source_of, place, traces, forcing, weight, last):
    mine, batch, _ = stay.shape
    piece = traces.shape[1]
    count = len(rows)

    def body(source_ref, stay_ref, got_ref, place_ref, traces_ref, forcing_ref, weight_ref, *refs):
        rows_refs, outs = refs[:count], refs[count:]
        dims = (((0,), (0,)), ((), ()))
        side = jnp.zeros((batch, piece), F32)
        for k in range(count):
            first, second = split(rows_refs[k][...])
            put = place_ref[source_ref[k]]
            side += lax.dot_general(first, put, dims, preferred_element_type=F32)
            side += lax.dot_general(second, put, dims, preferred_element_type=F32)
        for m in range(mine):
            at = slice(m * CHUNK, (m + 1) * CHUNK)
            total = stay_ref[m] + got_ref[m] + side[:, at]
            residual = forcing_ref[:, at] - total
            fresh = traces_ref[:, at] + weight_ref[:, at] * residual
            if last:
                outs[0][at, :] = fresh.T
                outs[1][at, :] = residual.T
            else:
                outs[0][:, at] = fresh

    shape = (piece, batch) if last else (batch, piece)
    out = (jax.ShapeDtypeStruct(shape, F32),) * (2 if last else 1)
    return pl.pallas_call(
        body,
        out_shape=out,
        in_specs=[smem()] + [vmem()] * (6 + count),
        out_specs=(vmem(),) * len(out),
        compiler_params=pltpu.CompilerParams(vmem_limit_bytes=6 << 20),
        cost_estimate=pl.CostEstimate(flops=2 * 10**8, bytes_accessed=0, transcendentals=0),
        name="update",
    )(source_of, stay, got, place, traces, forcing, weight, *rows)


def staged(boundary_block, schur_blocks, interface_rows, live_rows, row_scale, excitation):
    strips, piece, rows = boundary_block.shape
    wide = lax.axis_size("wide")
    grp = lax.axis_size("grp")
    outer = wide // 2
    owners = wide * grp
    share = schur_blocks.shape[1]
    wide_index = lax.axis_index("wide")
    grp_index = lax.axis_index("grp")
    me = wide_index * grp + grp_index
    as_array = lambda value: jnp.reshape(value, (1,)).astype(jnp.int32)
    group_array, panel_array = as_array(grp_index), as_array(lax.axis_index("narrow"))
    pair = [(0, 1), (1, 0)]

    def swap_inner(value):
        return lax.ppermute(value, "wide", [(i, i ^ 1) for i in range(wide)])

    def shift_outer(value, by):
        return lax.ppermute(value, "wide", [(i, (i + 2 * by) % wide) for i in range(wide)])

    def inner_first(value):
        return jnp.where(wide_index % 2 == 0, value, value[:, ::-1])

    forcing, weight, traces = begin(row_scale, excitation[0])

    slots = interface_rows[0]
    live = jnp.arange(slots.shape[0], dtype=jnp.int32) < live_rows[0]
    owner = slots // piece
    local = slots % piece
    column_of = jnp.where((owner % grp == grp_index) & live, (owner // grp) * piece + local, -1)[None, :]
    cap = (piece + owners - 1) // owners
    levels = jnp.arange(cap, dtype=jnp.int32)
    block_owner = owner.reshape(owners, share)
    block_rank = slot_ranks(block_owner)
    own_owner = lax.dynamic_slice_in_dim(block_owner, wide_index * grp, grp, 0)
    own_rank = lax.dynamic_slice_in_dim(block_rank, wide_index * grp, grp, 0)
    targets = jnp.arange(wide, dtype=jnp.int32) * grp + grp_index
    pick = (own_owner[None, :, None, :] == targets[:, None, None, None]) & (
        own_rank[None, :, None, :] == levels[None, None, :, None]
    )
    pick = pick[:, :, :, None, :] & jnp.eye(grp, dtype=bool)[None, :, None, :, None]
    pick = jnp.pad(pick, ((0, 0),) * 4 + ((0, CHUNK // grp - share),)).astype(BF16)
    pick = inner_first(pick.reshape(outer, 2, grp * cap, CHUNK)).reshape(outer, 2 * grp * cap, CHUNK)
    take = (
        (block_owner == me)[:, None, :]
        & (block_rank[:, None, :] == levels[None, :, None])
        & live.reshape(owners, 1, share)
    ).astype(BF16)
    landing = (local.reshape(owners, share)[..., None] == jnp.arange(piece, dtype=jnp.int32)).astype(BF16)
    place = jnp.einsum("jts,jsi->jti", take, landing, preferred_element_type=F32).astype(BF16)
    place = inner_first(place.reshape(outer, 2, grp * cap, piece)).reshape(outer, 2 * grp * cap, piece)

    schur_own = schur_blocks[0]
    schur_other = lax.ppermute(schur_own, "grp", pair)
    outer_index = wide_index // 2
    far = outer // 2
    near = [by for by in range(outer) if by != far]
    outer_of = tuple(
        jnp.stack([(outer_index + outer - by) % outer for by in group]).astype(jnp.int32) for group in (near, [far])
    )
    place_of = as_array(wide_index % 2)
    source_of = jnp.stack([(outer_index + outer - by) % outer for by in range(outer)]).astype(jnp.int32)
    target_of = jnp.stack([(outer_index + by) % outer for by in range(outer)]).astype(jnp.int32)
    column_of, pick, place, outer_of, place_of, source_of, target_of, panel_array, group_array, boundary_block = (
        lax.optimization_barrier(
            (column_of, pick, place, outer_of, place_of, source_of, target_of, panel_array, group_array, boundary_block)
        )
    )
    boundary_block = pltpu.with_memory_space_constraint(boundary_block, pltpu.HBM)
    chunks = rows // CHUNK
    many = 2
    high, low = [], []
    for first_chunk in range(0, chunks, many):
        more_high, more_low = tile_terms(boundary_block, first_chunk, many)
        high += more_high
        low += more_low
    more_high, more_low = schur_terms(schur_own, schur_other, column_of, group_array, strips, piece)
    high.append(more_high)
    low.append(more_low)

    for sweep in range(ITERS):
        shifted = [traces] + [shift_outer(traces, by) for by in range(1, outer)]
        pairs = [[block, swap_inner(block)] for block in shifted]
        near_blocks = [block for by in near for block in pairs[by]]
        keep, send, side = multiply(near_blocks, outer_of[0], place_of, group_array, high, low, ())
        (side,) = multiply(pairs[far], outer_of[1], place_of, group_array, high, low, (side,), main_rows=False)
        got_side = lax.ppermute(side, "grp", pair)
        own_rows, other_rows = pick_rows(side, got_side, pick, target_of)
        got_rows = swap_inner(other_rows)
        keep, send = multiply(pairs[far], outer_of[1], place_of, group_array, high, low, (keep, send), side_rows=False)
        got = lax.ppermute(send, "grp", pair)
        away, stay = gather_half(keep, got, panel_array)
        got = lax.ppermute(away, "narrow", pair)
        joined = join_rows(own_rows, got_rows)
        sides = [joined[0]] + [shift_outer(joined[by], by) for by in range(1, outer)]
        result = update(stay, got, sides, source_of, place, traces, forcing, weight, sweep == ITERS - 1)
        traces = result[0]
    return (result[0][None], result[1][None])
def on_device(boundary_block, schur_blocks, interface_rows, live_rows, row_scale, excitation):
    piece_rows = excitation.shape[1]
    wide_size = lax.axis_size("wide")
    grp_size = lax.axis_size("grp")
    blocks = wide_size * grp_size
    panel_size = blocks * piece_rows
    tile_block = boundary_block.reshape(-1, boundary_block.shape[2])
    row_weight = row_scale.reshape(piece_rows, 1)
    forcing = excitation[0]
    iface_size = interface_rows.shape[1]
    share_rows = schur_blocks.shape[1]
    sub_count = interface_rows.shape[0]
    row_group = lax.axis_index("wide") * grp_size + lax.axis_index("grp")
    positions = jnp.arange(iface_size, dtype=jnp.int32)
    live_mask = (positions[None, :] < live_rows[:, None]).astype(jnp.float32)
    own_rows = lax.dynamic_slice_in_dim(interface_rows, row_group * share_rows, share_rows, 1)
    slot_cap = (piece_rows + blocks - 1) // blocks
    targets = jnp.arange(blocks, dtype=jnp.int32)
    levels = jnp.arange(slot_cap, dtype=jnp.int32)
    send_owner = own_rows // piece_rows
    send_rank = slot_ranks(send_owner)
    send_pick = (
        (send_owner[:, None, None, :] == targets[None, :, None, None])
        & (send_rank[:, None, None, :] == levels[None, None, :, None])
    ).astype(jnp.float32)
    outgoing = jnp.einsum(
        "kots,ksm->oktm", send_pick, schur_blocks, precision=lax.Precision.HIGHEST
    )
    received = lax.all_to_all(outgoing, ("wide", "grp"), split_axis=0, concat_axis=0, tiled=True)
    block_rows = interface_rows.reshape(sub_count, blocks, share_rows)
    block_live = live_mask.reshape(sub_count, blocks, share_rows)
    block_owner = block_rows // piece_rows
    block_rank = slot_ranks(block_owner)
    take_pick = (
        (block_owner[:, :, None, :] == row_group)
        & (block_rank[:, :, None, :] == levels[None, None, :, None])
    ).astype(jnp.float32) * block_live[:, :, None, :]
    local_index = jnp.arange(piece_rows, dtype=jnp.int32)
    landing = ((block_rows % piece_rows)[..., None] == local_index).astype(jnp.float32)
    placement = jnp.einsum("kjts,kjsi->kjti", take_pick, landing, precision=lax.Precision.HIGHEST)
    traces = RELAX * row_weight * forcing
    residual = forcing
    for sweep in range(ITERS):
        wide_panel = lax.all_gather(traces[None], "wide", axis=0, tiled=True)
        full_panel = lax.all_gather(wide_panel[:, None], "grp", axis=1, tiled=True)
        stacked = wide_panel.reshape(-1, wide_panel.shape[-1])
        boundary = lax.psum_scatter(
            lax.dot_general(
                tile_block,
                stacked,
                (((0,), (0,)), ((), ())),
                precision=lax.Precision.HIGHEST,
                preferred_element_type=jnp.float32,
            ),
            ("narrow", "grp"),
            scatter_dimension=0,
            tiled=True,
        )
        flat_panel = full_panel.reshape(panel_size, -1)
        local_traces = jnp.take(flat_panel, interface_rows, axis=0) * live_mask[:, :, None]
        values = jnp.einsum(
            "jktm,kmr->kjtr", received, local_traces, precision=lax.Precision.HIGHEST
        )
        interface = jnp.einsum("kjti,kjtr->ir", placement, values, precision=lax.Precision.HIGHEST)
        residual = forcing - (boundary + interface)
        traces = traces + RELAX * row_weight * residual
    return (traces[None], residual[None])


def program(boundary_block, schur_blocks, interface_rows, live_rows, row_scale, excitation):
    strips, piece, rows = boundary_block.shape
    wide, narrow, grp = (lax.axis_size(name) for name in ("wide", "narrow", "grp"))
    regular = (
        wide % 2 == 0
        and wide & (wide - 1) == 0
        and narrow == 2
        and grp == 2
        and interface_rows.shape[0] == 1
        and piece % CHUNK == 0
        and rows == narrow * grp * piece
        and schur_blocks.shape[1] <= CHUNK // 2
        and excitation.shape[2] % 128 == 0
    )
    form = staged if regular else on_device
    return form(boundary_block, schur_blocks, interface_rows, live_rows, row_scale, excitation)


def solution(mesh):
    placed = (
        P(None, ("narrow", "grp"), "wide"),
        P("narrow", ("wide", "grp"), None),
        P("narrow", None),
        P("narrow"),
        P("wide", ("narrow", "grp")),
        P("wide", ("narrow", "grp"), None),
    )
    return jax.shard_map(
        program,
        mesh=mesh,
        in_specs=placed,
        out_specs=(P("wide", ("narrow", "grp"), None), P("wide", ("narrow", "grp"), None)),
        check_vma=False,
    )
```

```python
import jax
import jax.numpy as jnp
from jax import lax
from jax.experimental import pallas as pl
from jax.experimental.pallas import tpu as pltpu
from jax.sharding import PartitionSpec as P


ITERS = 3


RELAX = 0.35

CHUNK = 256
F32 = jnp.float32
BF16 = jnp.bfloat16


def split(value):
    high = value.astype(BF16)
    return high, (value - high.astype(F32)).astype(BF16)


def slot_ranks(owners):
    count = owners.shape[-1]
    same = owners[..., :, None] == owners[..., None, :]
    earlier = jnp.arange(count)[None, :] < jnp.arange(count)[:, None]
    return jnp.sum((same & earlier).astype(jnp.int32), axis=-1)


def vmem():
    return pl.BlockSpec(memory_space=pltpu.VMEM)


def smem():
    return pl.BlockSpec(memory_space=pltpu.SMEM)


def begin(row_scale, excitation):
    piece, batch = excitation.shape

    def body(scale_ref, excitation_ref, forcing_ref, weight_ref, traces_ref):
        weight_ref[...] = RELAX * scale_ref[...]
        forcing_ref[...] = excitation_ref[...].T
        traces_ref[...] = RELAX * scale_ref[...] * forcing_ref[...]

    wide = jax.ShapeDtypeStruct((batch, piece), F32)
    return pl.pallas_call(
        body,
        out_shape=(wide, jax.ShapeDtypeStruct((1, piece), F32), wide),
        in_specs=[vmem()] * 2,
        out_specs=(vmem(),) * 3,
        compiler_params=pltpu.CompilerParams(vmem_limit_bytes=4 << 20),
        name="begin",
    )(row_scale, excitation)


def tile_terms(boundary_block, first_chunk, many):
    strips, piece, _ = boundary_block.shape
    width = many * CHUNK
    depth = 3

    def body(b_ref, *refs):
        high_refs, low_refs = refs[:many], refs[many : 2 * many]
        buf, sems = refs[2 * many :]

        def copy(step, slot):
            return pltpu.make_async_copy(
                b_ref.at[step, :, pl.ds(first_chunk * CHUNK, width)], buf.at[slot], sems.at[slot]
            )

        for step in range(depth):
            copy(step, step).start()

        def one(step, carry):
            slot = lax.rem(step, depth)
            copy(step, slot).wait()
            inner = pl.ds(pl.multiple_of(lax.rem(step, 2) * piece, piece), piece)
            for n in range(many):
                high, low = split(buf[slot, :, n * CHUNK : (n + 1) * CHUNK])
                high_refs[n][step // 2, inner] = high
                low_refs[n][step // 2, inner] = low

            @pl.when(step + depth < strips)
            def _():
                copy(step + depth, slot).start()

            return carry

        lax.fori_loop(0, strips, one, 0)

    out = jax.ShapeDtypeStruct((strips // 2, 2 * piece, CHUNK), BF16)
    terms = pl.pallas_call(
        body,
        out_shape=(out,) * (2 * many),
        in_specs=[pl.BlockSpec(memory_space=pltpu.HBM)],
        out_specs=(vmem(),) * (2 * many),
        scratch_shapes=[pltpu.VMEM((depth, piece, width), F32), pltpu.SemaphoreType.DMA((depth,))],
        compiler_params=pltpu.CompilerParams(vmem_limit_bytes=16 << 20),
        cost_estimate=pl.CostEstimate(flops=4 * 10**9, bytes_accessed=0, transcendentals=0),
        name="tile_terms",
    )(boundary_block)
    return terms[:many], terms[many:]


def schur_terms(schur_own, schur_other, column_of, grp_index, strips, piece):
    share, slots = schur_own.shape
    half = CHUNK // 2

    def body(grp_ref, col_ref, own_ref, other_ref, high_ref, low_ref, s_high, s_low):
        s_high[...] = jnp.zeros(s_high.shape, BF16)
        s_low[...] = jnp.zeros(s_low.shape, BF16)
        group = grp_ref[0]
        for ref, at in ((own_ref, group), (other_ref, 1 - group)):
            high, low = split(ref[...])
            where = pl.ds(pl.multiple_of(at * half, half), share)
            s_high[where, :] = high
            s_low[where, :] = low

        def one(strip, carry):
            place = lax.broadcasted_iota(jnp.int32, (piece, slots), 0) + strip * piece
            hot = (place == col_ref[...]).astype(F32).astype(BF16)
            inner = pl.ds(pl.multiple_of(lax.rem(strip, 2) * piece, piece), piece)
            for term, out in ((s_high, high_ref), (s_low, low_ref)):
                value = lax.dot_general(hot, term[...], (((1,), (1,)), ((), ())), preferred_element_type=F32)
                out[strip // 2, inner] = value.astype(BF16)
            return carry

        lax.fori_loop(0, strips, one, 0)

    out = jax.ShapeDtypeStruct((strips // 2, 2 * piece, CHUNK), BF16)
    return pl.pallas_call(
        body,
        out_shape=(out, out),
        in_specs=[smem()] + [vmem()] * 3,
        out_specs=(vmem(),) * 2,
        scratch_shapes=[pltpu.VMEM((CHUNK, slots), BF16)] * 2,
        compiler_params=pltpu.CompilerParams(vmem_limit_bytes=10 << 20),
        cost_estimate=pl.CostEstimate(flops=2 * 10**9, bytes_accessed=0, transcendentals=0),
        name="schur_terms",
    )(grp_index, column_of, schur_own, schur_other)


def multiply(blocks, outer_of, place_of, grp_index, high, low, before, main_rows=True, side_rows=True):
    chunks = len(high) - 1
    pairs = len(blocks) // 2
    batch, piece = blocks[0].shape
    per_piece = piece // CHUNK
    kept = chunks // 2
    wanted = (list(range(chunks)) if main_rows else []) + ([chunks] if side_rows else [])

    def body(outer_ref, place_ref, grp_ref, *refs):
        take = iter(refs)
        block_refs = [next(take) for _ in range(2 * pairs)]
        high_refs = {n: next(take) for n in wanted}
        low_refs = {n: next(take) for n in wanted}
        old = [next(take) for _ in before]
        if main_rows:
            keep_ref, send_ref = next(take), next(take)
        if side_rows:
            side_ref = next(take)
        both, full = take
        group = grp_ref[0]
        swapped = place_ref[0]
        for j in range(2 * pairs):
            first, second = split(block_refs[j][...])
            at = pl.ds(pl.multiple_of(lax.rem(j + swapped, 2) * piece, piece), piece)
            both[j // 2, 0:batch, at] = first
            both[j // 2, batch : 2 * batch, at] = second

        def product(n):
            total = None
            for j in range(pairs):
                outer = outer_ref[j]
                top = jnp.dot(both[j], high_refs[n][outer], preferred_element_type=F32)
                bottom = jnp.dot(both[j, 0:batch, :], low_refs[n][outer], preferred_element_type=F32)
                value = top[:batch] + (top[batch:] + bottom)
                total = value if total is None else total + value
            return total

        if side_rows:
            value = product(chunks)
            side_ref[...] = old[-1][...] + value if before else value
        if main_rows:
            for n in range(chunks):
                full[n] = product(n)
            for m in range(kept):
                base = (m // per_piece) * 2 * per_piece + m % per_piece
                stays, goes = full[base + group * per_piece], full[base + (1 - group) * per_piece]
                keep_ref[m] = old[0][m] + stays if before else stays
                send_ref[m] = old[1][m] + goes if before else goes

    main = jax.ShapeDtypeStruct((kept, batch, CHUNK), F32)
    side = jax.ShapeDtypeStruct((batch, CHUNK), F32)
    flops = 6 * pairs * 2 * piece * batch * CHUNK * len(wanted)
    outs = ((main, main) if main_rows else ()) + ((side,) if side_rows else ())
    return pl.pallas_call(
        body,
        out_shape=outs,
        in_specs=[smem()] * 3 + [vmem()] * (2 * pairs + 2 * len(wanted) + len(before)),
        out_specs=(vmem(),) * len(outs),
        scratch_shapes=[
            pltpu.VMEM((pairs, 2 * batch, 2 * piece), BF16),
            pltpu.VMEM((chunks, batch, CHUNK), F32),
        ],
        compiler_params=pltpu.CompilerParams(vmem_limit_bytes=6 << 20),
        cost_estimate=pl.CostEstimate(flops=flops, bytes_accessed=0, transcendentals=0),
        name="multiply",
    )(outer_of, place_of, grp_index, *blocks, *(high[n] for n in wanted), *(low[n] for n in wanted), *before)


def gather_half(keep, got, narrow_index):
    kept, batch, _ = keep.shape
    mine = kept // 2

    def body(narrow_ref, keep_ref, got_ref, send_ref, stay_ref):
        panel = narrow_ref[0]
        for m in range(mine):
            send_ref[m] = keep_ref[(1 - panel) * mine + m] + got_ref[(1 - panel) * mine + m]
            stay_ref[m] = keep_ref[panel * mine + m] + got_ref[panel * mine + m]

    part = jax.ShapeDtypeStruct((mine, batch, CHUNK), F32)
    return pl.pallas_call(
        body,
        out_shape=(part, part),
        in_specs=[smem()] + [vmem()] * 2,
        out_specs=(vmem(),) * 2,
        compiler_params=pltpu.CompilerParams(vmem_limit_bytes=4 << 20),
        cost_estimate=pl.CostEstimate(flops=2 * 10**8, bytes_accessed=0, transcendentals=0),
        name="gather_half",
    )(narrow_index, keep, got)


def pick_rows(side, got_side, pick, target_of):
    outer, twice, _ = pick.shape
    cap = twice // 2
    batch = side.shape[0]

    def body(target_ref, side_ref, got_ref, pick_ref, own_ref, other_ref):
        first, second = split(side_ref[...] + got_ref[...])
        dims = (((1,), (1,)), ((), ()))
        for by in range(outer):
            chosen = pick_ref[target_ref[by]]
            rows = lax.dot_general(chosen, first, dims, preferred_element_type=F32)
            rows += lax.dot_general(chosen, second, dims, preferred_element_type=F32)
            own_ref[by] = rows[:cap]
            other_ref[by] = rows[cap:]

    rows = jax.ShapeDtypeStruct((outer, cap, batch), F32)
    return pl.pallas_call(
        body,
        out_shape=(rows, rows),
        in_specs=[smem()] + [vmem()] * 3,
        out_specs=(vmem(),) * 2,
        compiler_params=pltpu.CompilerParams(vmem_limit_bytes=4 << 20),
        cost_estimate=pl.CostEstimate(flops=2 * 10**8, bytes_accessed=0, transcendentals=0),
        name="pick_rows",
    )(target_of, side, got_side, pick)


def join_rows(own, got):
    outer, cap, batch = own.shape

    def body(own_ref, got_ref, *outs):
        for by in range(outer):
            outs[by][0:cap, :] = own_ref[by]
            outs[by][cap : 2 * cap, :] = got_ref[by]

    return pl.pallas_call(
        body,
        out_shape=(jax.ShapeDtypeStruct((2 * cap, batch), F32),) * outer,
        in_specs=[vmem()] * 2,
        out_specs=(vmem(),) * outer,
        compiler_params=pltpu.CompilerParams(vmem_limit_bytes=4 << 20),
        cost_estimate=pl.CostEstimate(flops=10**8, bytes_accessed=0, transcendentals=0),
        name="join_rows",
    )(own, got)


def update(stay, got, rows, source_of, place, traces, forcing, weight, last):
    mine, batch, _ = stay.shape
    piece = traces.shape[1]
    count = len(rows)

    def body(source_ref, stay_ref, got_ref, place_ref, traces_ref, forcing_ref, weight_ref, *refs):
        rows_refs, outs = refs[:count], refs[count:]
        dims = (((0,), (0,)), ((), ()))
        side = jnp.zeros((batch, piece), F32)
        for k in range(count):
            first, second = split(rows_refs[k][...])
            put = place_ref[source_ref[k]]
            side += lax.dot_general(first, put, dims, preferred_element_type=F32)
            side += lax.dot_general(second, put, dims, preferred_element_type=F32)
        for m in range(mine):
            at = slice(m * CHUNK, (m + 1) * CHUNK)
            total = stay_ref[m] + got_ref[m] + side[:, at]
            residual = forcing_ref[:, at] - total
            fresh = traces_ref[:, at] + weight_ref[:, at] * residual
            if last:
                outs[0][at, :] = fresh.T
                outs[1][at, :] = residual.T
            else:
                outs[0][:, at] = fresh

    shape = (piece, batch) if last else (batch, piece)
    out = (jax.ShapeDtypeStruct(shape, F32),) * (2 if last else 1)
    return pl.pallas_call(
        body,
        out_shape=out,
        in_specs=[smem()] + [vmem()] * (6 + count),
        out_specs=(vmem(),) * len(out),
        compiler_params=pltpu.CompilerParams(vmem_limit_bytes=6 << 20),
        cost_estimate=pl.CostEstimate(flops=2 * 10**8, bytes_accessed=0, transcendentals=0),
        name="update",
    )(source_of, stay, got, place, traces, forcing, weight, *rows)


def staged(boundary_block, schur_blocks, interface_rows, live_rows, row_scale, excitation):
    strips, piece, rows = boundary_block.shape
    wide = lax.axis_size("wide")
    grp = lax.axis_size("grp")
    outer = wide // 2
    owners = wide * grp
    share = schur_blocks.shape[1]
    wide_index = lax.axis_index("wide")
    grp_index = lax.axis_index("grp")
    me = wide_index * grp + grp_index
    as_array = lambda value: jnp.reshape(value, (1,)).astype(jnp.int32)
    group_array, panel_array = as_array(grp_index), as_array(lax.axis_index("narrow"))
    pair = [(0, 1), (1, 0)]

    def swap_inner(value):
        return lax.ppermute(value, "wide", [(i, i ^ 1) for i in range(wide)])

    def shift_outer(value, by):
        return lax.ppermute(value, "wide", [(i, (i + 2 * by) % wide) for i in range(wide)])

    def inner_first(value):
        return jnp.where(wide_index % 2 == 0, value, value[:, ::-1])

    forcing, weight, traces = begin(row_scale, excitation[0])

    slots = interface_rows[0]
    live = jnp.arange(slots.shape[0], dtype=jnp.int32) < live_rows[0]
    owner = slots // piece
    local = slots % piece
    column_of = jnp.where((owner % grp == grp_index) & live, (owner // grp) * piece + local, -1)[None, :]
    cap = (piece + owners - 1) // owners
    levels = jnp.arange(cap, dtype=jnp.int32)
    block_owner = owner.reshape(owners, share)
    block_rank = slot_ranks(block_owner)
    own_owner = lax.dynamic_slice_in_dim(block_owner, wide_index * grp, grp, 0)
    own_rank = lax.dynamic_slice_in_dim(block_rank, wide_index * grp, grp, 0)
    targets = jnp.arange(wide, dtype=jnp.int32) * grp + grp_index
    pick = (own_owner[None, :, None, :] == targets[:, None, None, None]) & (
        own_rank[None, :, None, :] == levels[None, None, :, None]
    )
    pick = pick[:, :, :, None, :] & jnp.eye(grp, dtype=bool)[None, :, None, :, None]
    pick = jnp.pad(pick, ((0, 0),) * 4 + ((0, CHUNK // grp - share),)).astype(BF16)
    pick = inner_first(pick.reshape(outer, 2, grp * cap, CHUNK)).reshape(outer, 2 * grp * cap, CHUNK)
    take = (
        (block_owner == me)[:, None, :]
        & (block_rank[:, None, :] == levels[None, :, None])
        & live.reshape(owners, 1, share)
    ).astype(BF16)
    landing = (local.reshape(owners, share)[..., None] == jnp.arange(piece, dtype=jnp.int32)).astype(BF16)
    place = jnp.einsum("jts,jsi->jti", take, landing, preferred_element_type=F32).astype(BF16)
    place = inner_first(place.reshape(outer, 2, grp * cap, piece)).reshape(outer, 2 * grp * cap, piece)

    schur_own = schur_blocks[0]
    schur_other = lax.ppermute(schur_own, "grp", pair)
    outer_index = wide_index // 2
    far = outer // 2
    near = [by for by in range(outer) if by != far]
    outer_of = tuple(as_array((outer_index + outer - by) % outer) for by in range(outer))
    place_of = as_array(wide_index % 2)
    source_of = jnp.stack([(outer_index + outer - by) % outer for by in range(outer)]).astype(jnp.int32)
    target_of = jnp.stack([(outer_index + by) % outer for by in range(outer)]).astype(jnp.int32)
    column_of, pick, place, outer_of, place_of, source_of, target_of, panel_array, group_array, boundary_block = (
        lax.optimization_barrier(
            (column_of, pick, place, outer_of, place_of, source_of, target_of, panel_array, group_array, boundary_block)
        )
    )
    boundary_block = pltpu.with_memory_space_constraint(boundary_block, pltpu.HBM)
    chunks = rows // CHUNK
    many = chunks
    high, low = [], []
    for first_chunk in range(0, chunks, many):
        more_high, more_low = tile_terms(boundary_block, first_chunk, many)
        high += more_high
        low += more_low
    more_high, more_low = schur_terms(schur_own, schur_other, column_of, group_array, strips, piece)
    high.append(more_high)
    low.append(more_low)

    def one_sweep(sweep):
        pairs = []
        for by in range(outer):
            block = traces if by == 0 else shift_outer(traces, by)
            pairs.append([block, swap_inner(block)])
        partial = ()
        for by in near:
            partial = multiply(pairs[by], outer_of[by], place_of, group_array, high, low, partial)
        keep, send, side = partial
        (side,) = multiply(pairs[far], outer_of[far], place_of, group_array, high, low, (side,), main_rows=False)
        got_side = lax.ppermute(side, "grp", pair)
        own_rows, other_rows = pick_rows(side, got_side, pick, target_of)
        got_rows = swap_inner(other_rows)
        keep, send = multiply(pairs[far], outer_of[far], place_of, group_array, high, low, (keep, send), side_rows=False)
        got = lax.ppermute(send, "grp", pair)
        away, stay = gather_half(keep, got, panel_array)
        got = lax.ppermute(away, "narrow", pair)
        joined = join_rows(own_rows, got_rows)
        sides = [joined[0]]
        for by in range(1, outer):
            sides.append(shift_outer(joined[by], by))
        return update(stay, got, sides, source_of, place, traces, forcing, weight, sweep == ITERS - 1)

    for sweep in range(ITERS):
        result = one_sweep(sweep)
        traces = result[0]
    return (result[0][None], result[1][None])


def on_device(boundary_block, schur_blocks, interface_rows, live_rows, row_scale, excitation):
    piece_rows = excitation.shape[1]
    wide_size = lax.axis_size("wide")
    grp_size = lax.axis_size("grp")
    blocks = wide_size * grp_size
    panel_size = blocks * piece_rows
    tile_block = boundary_block.reshape(-1, boundary_block.shape[2])
    row_weight = row_scale.reshape(piece_rows, 1)
    forcing = excitation[0]
    iface_size = interface_rows.shape[1]
    share_rows = schur_blocks.shape[1]
    sub_count = interface_rows.shape[0]
    row_group = lax.axis_index("wide") * grp_size + lax.axis_index("grp")
    positions = jnp.arange(iface_size, dtype=jnp.int32)
    live_mask = (positions[None, :] < live_rows[:, None]).astype(jnp.float32)
    own_rows = lax.dynamic_slice_in_dim(interface_rows, row_group * share_rows, share_rows, 1)
    slot_cap = (piece_rows + blocks - 1) // blocks
    targets = jnp.arange(blocks, dtype=jnp.int32)
    levels = jnp.arange(slot_cap, dtype=jnp.int32)
    send_owner = own_rows // piece_rows
    send_rank = slot_ranks(send_owner)
    send_pick = (
        (send_owner[:, None, None, :] == targets[None, :, None, None])
        & (send_rank[:, None, None, :] == levels[None, None, :, None])
    ).astype(jnp.float32)
    outgoing = jnp.einsum(
        "kots,ksm->oktm", send_pick, schur_blocks, precision=lax.Precision.HIGHEST
    )
    received = lax.all_to_all(outgoing, ("wide", "grp"), split_axis=0, concat_axis=0, tiled=True)
    block_rows = interface_rows.reshape(sub_count, blocks, share_rows)
    block_live = live_mask.reshape(sub_count, blocks, share_rows)
    block_owner = block_rows // piece_rows
    block_rank = slot_ranks(block_owner)
    take_pick = (
        (block_owner[:, :, None, :] == row_group)
        & (block_rank[:, :, None, :] == levels[None, None, :, None])
    ).astype(jnp.float32) * block_live[:, :, None, :]
    local_index = jnp.arange(piece_rows, dtype=jnp.int32)
    landing = ((block_rows % piece_rows)[..., None] == local_index).astype(jnp.float32)
    placement = jnp.einsum("kjts,kjsi->kjti", take_pick, landing, precision=lax.Precision.HIGHEST)
    traces = RELAX * row_weight * forcing
    residual = forcing
    for _ in range(ITERS):
        wide_panel = lax.all_gather(traces[None], "wide", axis=0, tiled=True)
        full_panel = lax.all_gather(wide_panel[:, None], "grp", axis=1, tiled=True)
        stacked = wide_panel.reshape(-1, wide_panel.shape[-1])
        boundary = lax.psum_scatter(
            lax.dot_general(
                tile_block,
                stacked,
                (((0,), (0,)), ((), ())),
                precision=lax.Precision.HIGHEST,
                preferred_element_type=jnp.float32,
            ),
            ("narrow", "grp"),
            scatter_dimension=0,
            tiled=True,
        )
        flat_panel = full_panel.reshape(panel_size, -1)
        local_traces = jnp.take(flat_panel, interface_rows, axis=0) * live_mask[:, :, None]
        values = jnp.einsum(
            "jktm,kmr->kjtr", received, local_traces, precision=lax.Precision.HIGHEST
        )
        interface = jnp.einsum("kjti,kjtr->ir", placement, values, precision=lax.Precision.HIGHEST)
        residual = forcing - (boundary + interface)
        traces = traces + RELAX * row_weight * residual
    return (traces[None], residual[None])


def program(boundary_block, schur_blocks, interface_rows, live_rows, row_scale, excitation):
    _, piece, rows = boundary_block.shape
    wide, narrow, grp = (lax.axis_size(name) for name in ("wide", "narrow", "grp"))
    regular = (
        wide % 2 == 0
        and wide & (wide - 1) == 0
        and narrow == 2
        and grp == 2
        and interface_rows.shape[0] == 1
        and piece % CHUNK == 0
        and rows == narrow * grp * piece
        and schur_blocks.shape[1] <= CHUNK // 2
        and excitation.shape[2] % 128 == 0
    )
    form = staged if regular else on_device
    return form(boundary_block, schur_blocks, interface_rows, live_rows, row_scale, excitation)


def solution(mesh):
    placed = (
        P(None, ("narrow", "grp"), "wide"),
        P("narrow", ("wide", "grp"), None),
        P("narrow", None),
        P("narrow"),
        P("wide", ("narrow", "grp")),
        P("wide", ("narrow", "grp"), None),
    )
    return jax.shard_map(
        program,
        mesh=mesh,
        in_specs=placed,
        out_specs=(P("wide", ("narrow", "grp"), None), P("wide", ("narrow", "grp"), None)),
        check_vma=False,
    )
```

```python
import jax
import jax.numpy as jnp
from jax import lax
from jax.experimental import pallas as pl
from jax.experimental.pallas import tpu as pltpu
from jax.sharding import PartitionSpec as P


ITERS = 3


RELAX = 0.35

CHUNK = 256
F32 = jnp.float32
BF16 = jnp.bfloat16


def split(value):
    high = value.astype(BF16)
    return high, (value - high.astype(F32)).astype(BF16)


def slot_ranks(owners):
    count = owners.shape[-1]
    same = owners[..., :, None] == owners[..., None, :]
    earlier = jnp.arange(count)[None, :] < jnp.arange(count)[:, None]
    return jnp.sum((same & earlier).astype(jnp.int32), axis=-1)


def vmem():
    return pl.BlockSpec(memory_space=pltpu.VMEM)


def smem():
    return pl.BlockSpec(memory_space=pltpu.SMEM)


def begin(row_scale, excitation):
    piece, batch = excitation.shape

    def body(scale_hbm, excitation_hbm, forcing_ref, weight_ref, traces_ref, scale_ref, excitation_ref, sems):
        copies = [
            pltpu.make_async_copy(excitation_hbm, excitation_ref, sems.at[0]),
            pltpu.make_async_copy(scale_hbm, scale_ref, sems.at[1]),
        ]
        for copy in copies:
            copy.start()
        for copy in copies:
            copy.wait()
        weight_ref[...] = RELAX * scale_ref[...]
        forcing_ref[...] = excitation_ref[...].T
        traces_ref[...] = RELAX * scale_ref[...] * forcing_ref[...]

    wide = jax.ShapeDtypeStruct((batch, piece), F32)
    hbm = pl.BlockSpec(memory_space=pltpu.HBM)
    return pl.pallas_call(
        body,
        out_shape=(wide, jax.ShapeDtypeStruct((1, piece), F32), wide),
        in_specs=[hbm, hbm],
        out_specs=(vmem(),) * 3,
        scratch_shapes=[
            pltpu.VMEM((1, piece), F32),
            pltpu.VMEM((piece, batch), F32),
            pltpu.SemaphoreType.DMA((2,)),
        ],
        compiler_params=pltpu.CompilerParams(vmem_limit_bytes=4 << 20),
        name="begin",
    )(pltpu.with_memory_space_constraint(row_scale, pltpu.HBM), pltpu.with_memory_space_constraint(excitation, pltpu.HBM))


def tile_terms(boundary_block, first_chunk, many):
    strips, piece, _ = boundary_block.shape
    width = many * CHUNK
    parts = 2
    part = piece // parts
    steps = strips * parts
    depth = 6

    def body(b_ref, *refs):
        high_refs, low_refs = refs[:many], refs[many : 2 * many]
        buf, sems = refs[2 * many :]

        def copy(step, slot):
            where = pl.ds(pl.multiple_of((step % parts) * part, part), part)
            return pltpu.make_async_copy(
                b_ref.at[step // parts, where, pl.ds(first_chunk * CHUNK, width)], buf.at[slot], sems.at[slot]
            )

        for step in range(depth):
            copy(step, step).start()

        def one(step, carry):
            slot = lax.rem(step, depth)
            copy(step, slot).wait()
            inner = pl.ds(pl.multiple_of(lax.rem(step, 2 * parts) * part, part), part)
            for n in range(many):
                high, low = split(buf[slot, :, n * CHUNK : (n + 1) * CHUNK])
                high_refs[n][step // (2 * parts), inner] = high
                low_refs[n][step // (2 * parts), inner] = low

            @pl.when(step + depth < steps)
            def _():
                copy(step + depth, slot).start()

            return carry

        lax.fori_loop(0, steps, one, 0)

    out = jax.ShapeDtypeStruct((strips // 2, 2 * piece, CHUNK), BF16)
    terms = pl.pallas_call(
        body,
        out_shape=(out,) * (2 * many),
        in_specs=[pl.BlockSpec(memory_space=pltpu.HBM)],
        out_specs=(vmem(),) * (2 * many),
        scratch_shapes=[pltpu.VMEM((depth, part, width), F32), pltpu.SemaphoreType.DMA((depth,))],
        compiler_params=pltpu.CompilerParams(vmem_limit_bytes=16 << 20),
        cost_estimate=pl.CostEstimate(flops=4 * 10**9, bytes_accessed=0, transcendentals=0),
        name="tile_terms",
    )(boundary_block)
    return terms[:many], terms[many:]


def schur_terms(schur_own, schur_other, column_of, grp_index, strips, piece):
    share, slots = schur_own.shape
    half = CHUNK // 2

    def body(grp_ref, col_ref, own_ref, other_ref, high_ref, low_ref, s_high, s_low):
        s_high[...] = jnp.zeros(s_high.shape, BF16)
        s_low[...] = jnp.zeros(s_low.shape, BF16)
        group = grp_ref[0]
        for ref, at in ((own_ref, group), (other_ref, 1 - group)):
            high, low = split(ref[...])
            where = pl.ds(pl.multiple_of(at * half, half), share)
            s_high[where, :] = high
            s_low[where, :] = low

        def one(strip, carry):
            place = lax.broadcasted_iota(jnp.int32, (piece, slots), 0) + strip * piece
            hot = (place == col_ref[...]).astype(F32).astype(BF16)
            inner = pl.ds(pl.multiple_of(lax.rem(strip, 2) * piece, piece), piece)
            for term, out in ((s_high, high_ref), (s_low, low_ref)):
                value = lax.dot_general(hot, term[...], (((1,), (1,)), ((), ())), preferred_element_type=F32)
                out[strip // 2, inner] = value.astype(BF16)
            return carry

        lax.fori_loop(0, strips, one, 0)

    out = jax.ShapeDtypeStruct((strips // 2, 2 * piece, CHUNK), BF16)
    return pl.pallas_call(
        body,
        out_shape=(out, out),
        in_specs=[smem()] + [vmem()] * 3,
        out_specs=(vmem(),) * 2,
        scratch_shapes=[pltpu.VMEM((CHUNK, slots), BF16)] * 2,
        compiler_params=pltpu.CompilerParams(vmem_limit_bytes=10 << 20),
        cost_estimate=pl.CostEstimate(flops=2 * 10**9, bytes_accessed=0, transcendentals=0),
        name="schur_terms",
    )(grp_index, column_of, schur_own, schur_other)


def multiply(blocks, outer_of, place_of, grp_index, high, low, before, main_rows=True, side_rows=True):
    chunks = len(high) - 1
    pairs = len(blocks) // 2
    batch, piece = blocks[0].shape
    per_piece = piece // CHUNK
    kept = chunks // 2
    wanted = (list(range(chunks)) if main_rows else []) + ([chunks] if side_rows else [])

    def body(outer_ref, place_ref, grp_ref, *refs):
        take = iter(refs)
        block_refs = [next(take) for _ in range(2 * pairs)]
        high_refs = {n: next(take) for n in wanted}
        low_refs = {n: next(take) for n in wanted}
        old = [next(take) for _ in before]
        if main_rows:
            keep_ref, send_ref = next(take), next(take)
        if side_rows:
            side_ref = next(take)
        both, full = take
        group = grp_ref[0]
        swapped = place_ref[0]
        for j in range(2 * pairs):
            first, second = split(block_refs[j][...])
            at = pl.ds(pl.multiple_of(lax.rem(j + swapped, 2) * piece, piece), piece)
            both[j // 2, 0:batch, at] = first
            both[j // 2, batch : 2 * batch, at] = second

        def product(n):
            total = None
            for j in range(pairs):
                outer = outer_ref[j]
                top = jnp.dot(both[j], high_refs[n][outer], preferred_element_type=F32)
                bottom = jnp.dot(both[j, 0:batch, :], low_refs[n][outer], preferred_element_type=F32)
                value = top[:batch] + (top[batch:] + bottom)
                total = value if total is None else total + value
            return total

        if side_rows:
            value = product(chunks)
            side_ref[...] = old[-1][...] + value if before else value
        if main_rows:
            for n in range(chunks):
                full[n] = product(n)
            for m in range(kept):
                base = (m // per_piece) * 2 * per_piece + m % per_piece
                stays, goes = full[base + group * per_piece], full[base + (1 - group) * per_piece]
                keep_ref[m] = old[0][m] + stays if before else stays
                send_ref[m] = old[1][m] + goes if before else goes

    main = jax.ShapeDtypeStruct((kept, batch, CHUNK), F32)
    side = jax.ShapeDtypeStruct((batch, CHUNK), F32)
    flops = 6 * pairs * 2 * piece * batch * CHUNK * len(wanted)
    outs = ((main, main) if main_rows else ()) + ((side,) if side_rows else ())
    return pl.pallas_call(
        body,
        out_shape=outs,
        in_specs=[smem()] * 3 + [vmem()] * (2 * pairs + 2 * len(wanted) + len(before)),
        out_specs=(vmem(),) * len(outs),
        scratch_shapes=[
            pltpu.VMEM((pairs, 2 * batch, 2 * piece), BF16),
            pltpu.VMEM((chunks, batch, CHUNK), F32),
        ],
        compiler_params=pltpu.CompilerParams(vmem_limit_bytes=6 << 20),
        cost_estimate=pl.CostEstimate(flops=flops, bytes_accessed=0, transcendentals=0),
        name="multiply",
    )(outer_of, place_of, grp_index, *blocks, *(high[n] for n in wanted), *(low[n] for n in wanted), *before)


def gather_half(keep, got, narrow_index):
    kept, batch, _ = keep.shape
    mine = kept // 2

    def body(narrow_ref, keep_ref, got_ref, send_ref, stay_ref):
        panel = narrow_ref[0]
        for m in range(mine):
            send_ref[m] = keep_ref[(1 - panel) * mine + m] + got_ref[(1 - panel) * mine + m]
            stay_ref[m] = keep_ref[panel * mine + m] + got_ref[panel * mine + m]

    part = jax.ShapeDtypeStruct((mine, batch, CHUNK), F32)
    return pl.pallas_call(
        body,
        out_shape=(part, part),
        in_specs=[smem()] + [vmem()] * 2,
        out_specs=(vmem(),) * 2,
        compiler_params=pltpu.CompilerParams(vmem_limit_bytes=4 << 20),
        cost_estimate=pl.CostEstimate(flops=2 * 10**8, bytes_accessed=0, transcendentals=0),
        name="gather_half",
    )(narrow_index, keep, got)


def pick_rows(side, got_side, pick, target_of):
    outer, twice, _ = pick.shape
    cap = twice // 2
    batch = side.shape[0]

    def body(target_ref, side_ref, got_ref, pick_ref, own_ref, other_ref):
        first, second = split(side_ref[...] + got_ref[...])
        dims = (((1,), (1,)), ((), ()))
        for by in range(outer):
            chosen = pick_ref[target_ref[by]]
            rows = lax.dot_general(chosen, first, dims, preferred_element_type=F32)
            rows += lax.dot_general(chosen, second, dims, preferred_element_type=F32)
            own_ref[by] = rows[:cap]
            other_ref[by] = rows[cap:]

    rows = jax.ShapeDtypeStruct((outer, cap, batch), F32)
    return pl.pallas_call(
        body,
        out_shape=(rows, rows),
        in_specs=[smem()] + [vmem()] * 3,
        out_specs=(vmem(),) * 2,
        compiler_params=pltpu.CompilerParams(vmem_limit_bytes=4 << 20),
        cost_estimate=pl.CostEstimate(flops=2 * 10**8, bytes_accessed=0, transcendentals=0),
        name="pick_rows",
    )(target_of, side, got_side, pick)


def join_rows(own, got):
    outer, cap, batch = own.shape

    def body(own_ref, got_ref, *outs):
        for by in range(outer):
            outs[by][0:cap, :] = own_ref[by]
            outs[by][cap : 2 * cap, :] = got_ref[by]

    return pl.pallas_call(
        body,
        out_shape=(jax.ShapeDtypeStruct((2 * cap, batch), F32),) * outer,
        in_specs=[vmem()] * 2,
        out_specs=(vmem(),) * outer,
        compiler_params=pltpu.CompilerParams(vmem_limit_bytes=4 << 20),
        cost_estimate=pl.CostEstimate(flops=10**8, bytes_accessed=0, transcendentals=0),
        name="join_rows",
    )(own, got)


def update(stay, got, rows, source_of, place, traces, forcing, weight, last):
    mine, batch, _ = stay.shape
    piece = traces.shape[1]
    count = len(rows)

    def body(source_ref, stay_ref, got_ref, place_ref, traces_ref, forcing_ref, weight_ref, *refs):
        rows_refs, outs = refs[:count], refs[count:]
        dims = (((0,), (0,)), ((), ()))
        side = jnp.zeros((batch, piece), F32)
        for k in range(count):
            first, second = split(rows_refs[k][...])
            put = place_ref[source_ref[k]]
            side += lax.dot_general(first, put, dims, preferred_element_type=F32)
            side += lax.dot_general(second, put, dims, preferred_element_type=F32)
        for m in range(mine):
            at = slice(m * CHUNK, (m + 1) * CHUNK)
            total = stay_ref[m] + got_ref[m] + side[:, at]
            residual = forcing_ref[:, at] - total
            fresh = traces_ref[:, at] + weight_ref[:, at] * residual
            if last:
                outs[0][at, :] = fresh.T
                outs[1][at, :] = residual.T
            else:
                outs[0][:, at] = fresh

    shape = (piece, batch) if last else (batch, piece)
    out = (jax.ShapeDtypeStruct(shape, F32),) * (2 if last else 1)
    return pl.pallas_call(
        body,
        out_shape=out,
        in_specs=[smem()] + [vmem()] * (6 + count),
        out_specs=(vmem(),) * len(out),
        compiler_params=pltpu.CompilerParams(vmem_limit_bytes=6 << 20),
        cost_estimate=pl.CostEstimate(flops=2 * 10**8, bytes_accessed=0, transcendentals=0),
        name="update",
    )(source_of, stay, got, place, traces, forcing, weight, *rows)


def staged(boundary_block, schur_blocks, interface_rows, live_rows, row_scale, excitation):
    strips, piece, rows = boundary_block.shape
    wide = lax.axis_size("wide")
    grp = lax.axis_size("grp")
    outer = wide // 2
    owners = wide * grp
    share = schur_blocks.shape[1]
    wide_index = lax.axis_index("wide")
    grp_index = lax.axis_index("grp")
    me = wide_index * grp + grp_index
    as_array = lambda value: jnp.reshape(value, (1,)).astype(jnp.int32)
    group_array, panel_array = as_array(grp_index), as_array(lax.axis_index("narrow"))
    pair = [(0, 1), (1, 0)]

    def swap_inner(value):
        return lax.ppermute(value, "wide", [(i, i ^ 1) for i in range(wide)])

    def shift_outer(value, by):
        return lax.ppermute(value, "wide", [(i, (i + 2 * by) % wide) for i in range(wide)])

    def inner_first(value):
        return jnp.where(wide_index % 2 == 0, value, value[:, ::-1])

    forcing, weight, traces = begin(row_scale, excitation[0])

    slots = interface_rows[0]
    live = jnp.arange(slots.shape[0], dtype=jnp.int32) < live_rows[0]
    owner = slots // piece
    local = slots % piece
    column_of = jnp.where((owner % grp == grp_index) & live, (owner // grp) * piece + local, -1)[None, :]
    cap = (piece + owners - 1) // owners
    levels = jnp.arange(cap, dtype=jnp.int32)
    block_owner = owner.reshape(owners, share)
    block_rank = slot_ranks(block_owner)
    own_owner = lax.dynamic_slice_in_dim(block_owner, wide_index * grp, grp, 0)
    own_rank = lax.dynamic_slice_in_dim(block_rank, wide_index * grp, grp, 0)
    targets = jnp.arange(wide, dtype=jnp.int32) * grp + grp_index
    pick = (own_owner[None, :, None, :] == targets[:, None, None, None]) & (
        own_rank[None, :, None, :] == levels[None, None, :, None]
    )
    pick = pick[:, :, :, None, :] & jnp.eye(grp, dtype=bool)[None, :, None, :, None]
    pick = jnp.pad(pick, ((0, 0),) * 4 + ((0, CHUNK // grp - share),)).astype(BF16)
    pick = inner_first(pick.reshape(outer, 2, grp * cap, CHUNK)).reshape(outer, 2 * grp * cap, CHUNK)
    take = (
        (block_owner == me)[:, None, :]
        & (block_rank[:, None, :] == levels[None, :, None])
        & live.reshape(owners, 1, share)
    ).astype(BF16)
    landing = (local.reshape(owners, share)[..., None] == jnp.arange(piece, dtype=jnp.int32)).astype(BF16)
    place = jnp.einsum("jts,jsi->jti", take, landing, preferred_element_type=F32).astype(BF16)
    place = inner_first(place.reshape(outer, 2, grp * cap, piece)).reshape(outer, 2 * grp * cap, piece)

    schur_own = schur_blocks[0]
    schur_other = lax.ppermute(schur_own, "grp", pair)
    outer_index = wide_index // 2
    far = outer // 2
    near = [by for by in range(outer) if by != far]
    outer_of = tuple(as_array((outer_index + outer - by) % outer) for by in range(outer))
    place_of = as_array(wide_index % 2)
    source_of = jnp.stack([(outer_index + outer - by) % outer for by in range(outer)]).astype(jnp.int32)
    target_of = jnp.stack([(outer_index + by) % outer for by in range(outer)]).astype(jnp.int32)
    column_of, pick, place, outer_of, place_of, source_of, target_of, panel_array, group_array, boundary_block = (
        lax.optimization_barrier(
            (column_of, pick, place, outer_of, place_of, source_of, target_of, panel_array, group_array, boundary_block)
        )
    )
    boundary_block = pltpu.with_memory_space_constraint(boundary_block, pltpu.HBM)
    chunks = rows // CHUNK
    many = chunks
    high, low = [], []
    for first_chunk in range(0, chunks, many):
        more_high, more_low = tile_terms(boundary_block, first_chunk, many)
        high += more_high
        low += more_low
    more_high, more_low = schur_terms(schur_own, schur_other, column_of, group_array, strips, piece)
    high.append(more_high)
    low.append(more_low)

    def one_sweep(sweep):
        pairs = []
        for by in range(outer):
            block = traces if by == 0 else shift_outer(traces, by)
            pairs.append([block, swap_inner(block)])
        partial = ()
        for by in near:
            partial = multiply(pairs[by], outer_of[by], place_of, group_array, high, low, partial)
        keep, send, side = partial
        (side,) = multiply(pairs[far], outer_of[far], place_of, group_array, high, low, (side,), main_rows=False)
        got_side = lax.ppermute(side, "grp", pair)
        own_rows, other_rows = pick_rows(side, got_side, pick, target_of)
        got_rows = swap_inner(other_rows)
        keep, send = multiply(pairs[far], outer_of[far], place_of, group_array, high, low, (keep, send), side_rows=False)
        got = lax.ppermute(send, "grp", pair)
        away, stay = gather_half(keep, got, panel_array)
        got = lax.ppermute(away, "narrow", pair)
        joined = join_rows(own_rows, got_rows)
        sides = [joined[0]]
        for by in range(1, outer):
            sides.append(shift_outer(joined[by], by))
        return update(stay, got, sides, source_of, place, traces, forcing, weight, sweep == ITERS - 1)

    for sweep in range(ITERS):
        result = one_sweep(sweep)
        traces = result[0]
    return (result[0][None], result[1][None])


def on_device(boundary_block, schur_blocks, interface_rows, live_rows, row_scale, excitation):
    piece_rows = excitation.shape[1]
    wide_size = lax.axis_size("wide")
    grp_size = lax.axis_size("grp")
    blocks = wide_size * grp_size
    panel_size = blocks * piece_rows
    tile_block = boundary_block.reshape(-1, boundary_block.shape[2])
    row_weight = row_scale.reshape(piece_rows, 1)
    forcing = excitation[0]
    iface_size = interface_rows.shape[1]
    share_rows = schur_blocks.shape[1]
    sub_count = interface_rows.shape[0]
    row_group = lax.axis_index("wide") * grp_size + lax.axis_index("grp")
    positions = jnp.arange(iface_size, dtype=jnp.int32)
    live_mask = (positions[None, :] < live_rows[:, None]).astype(jnp.float32)
    own_rows = lax.dynamic_slice_in_dim(interface_rows, row_group * share_rows, share_rows, 1)
    slot_cap = (piece_rows + blocks - 1) // blocks
    targets = jnp.arange(blocks, dtype=jnp.int32)
    levels = jnp.arange(slot_cap, dtype=jnp.int32)
    send_owner = own_rows // piece_rows
    send_rank = slot_ranks(send_owner)
    send_pick = (
        (send_owner[:, None, None, :] == targets[None, :, None, None])
        & (send_rank[:, None, None, :] == levels[None, None, :, None])
    ).astype(jnp.float32)
    outgoing = jnp.einsum(
        "kots,ksm->oktm", send_pick, schur_blocks, precision=lax.Precision.HIGHEST
    )
    received = lax.all_to_all(outgoing, ("wide", "grp"), split_axis=0, concat_axis=0, tiled=True)
    block_rows = interface_rows.reshape(sub_count, blocks, share_rows)
    block_live = live_mask.reshape(sub_count, blocks, share_rows)
    block_owner = block_rows // piece_rows
    block_rank = slot_ranks(block_owner)
    take_pick = (
        (block_owner[:, :, None, :] == row_group)
        & (block_rank[:, :, None, :] == levels[None, None, :, None])
    ).astype(jnp.float32) * block_live[:, :, None, :]
    local_index = jnp.arange(piece_rows, dtype=jnp.int32)
    landing = ((block_rows % piece_rows)[..., None] == local_index).astype(jnp.float32)
    placement = jnp.einsum("kjts,kjsi->kjti", take_pick, landing, precision=lax.Precision.HIGHEST)
    traces = RELAX * row_weight * forcing
    residual = forcing
    for _ in range(ITERS):
        wide_panel = lax.all_gather(traces[None], "wide", axis=0, tiled=True)
        full_panel = lax.all_gather(wide_panel[:, None], "grp", axis=1, tiled=True)
        stacked = wide_panel.reshape(-1, wide_panel.shape[-1])
        boundary = lax.psum_scatter(
            lax.dot_general(
                tile_block,
                stacked,
                (((0,), (0,)), ((), ())),
                precision=lax.Precision.HIGHEST,
                preferred_element_type=jnp.float32,
            ),
            ("narrow", "grp"),
            scatter_dimension=0,
            tiled=True,
        )
        flat_panel = full_panel.reshape(panel_size, -1)
        local_traces = jnp.take(flat_panel, interface_rows, axis=0) * live_mask[:, :, None]
        values = jnp.einsum(
            "jktm,kmr->kjtr", received, local_traces, precision=lax.Precision.HIGHEST
        )
        interface = jnp.einsum("kjti,kjtr->ir", placement, values, precision=lax.Precision.HIGHEST)
        residual = forcing - (boundary + interface)
        traces = traces + RELAX * row_weight * residual
    return (traces[None], residual[None])


def program(boundary_block, schur_blocks, interface_rows, live_rows, row_scale, excitation):
    _, piece, rows = boundary_block.shape
    wide, narrow, grp = (lax.axis_size(name) for name in ("wide", "narrow", "grp"))
    regular = (
        wide % 2 == 0
        and wide & (wide - 1) == 0
        and narrow == 2
        and grp == 2
        and interface_rows.shape[0] == 1
        and piece % CHUNK == 0
        and rows == narrow * grp * piece
        and schur_blocks.shape[1] <= CHUNK // 2
        and excitation.shape[2] % 128 == 0
    )
    form = staged if regular else on_device
    return form(boundary_block, schur_blocks, interface_rows, live_rows, row_scale, excitation)


def solution(mesh):
    placed = (
        P(None, ("narrow", "grp"), "wide"),
        P("narrow", ("wide", "grp"), None),
        P("narrow", None),
        P("narrow"),
        P("wide", ("narrow", "grp")),
        P("wide", ("narrow", "grp"), None),
    )
    return jax.shard_map(
        program,
        mesh=mesh,
        in_specs=placed,
        out_specs=(P("wide", ("narrow", "grp"), None), P("wide", ("narrow", "grp"), None)),
        check_vma=False,
    )
```
